256 devices in a mesh: freq: 32 (over z, x_lo, core), rcv: 8 (over x_hi, y).
Axes of the slice: x: 4 (x_hi: 2, x_lo: 2; x = x_hi * 2 + x_lo), y: 4, z: 8, core: 2. Of those that a mesh axis runs over, the one named last changes fastest.
Arguments:
- reflection: bfloat16 [2, 128, 768, 768], P(None, 'freq', 'rcv'), may hold values from -0.21875 to 0.21875
- direct: bfloat16 [768, 128, 512], P(('rcv', 'freq')), may hold values from -6 to 6
- onset: int32 [768, 128], P(('rcv', 'freq')), may hold values from 128 to 383
Outputs:
- focus_plus: bfloat16 [768, 128, 512], P(('rcv', 'freq'))
- focus_minus: bfloat16 [768, 128, 512], P(('rcv', 'freq'))
- correlation: float32 [2, 128, 128, 128], P(None, 'freq', 'rcv')
The draws below stay inside these ranges and needn't reach their ends.
All inputs are finite; a program needn't handle non-finite values.
Results may differ from the reference program's by a relative error of at most 0.019.
Values may be sent and summed in bfloat16 or wider, within the bound.
No kernel may reach another device: no remote copies, remote signals or barrier semaphores. Data moves between devices by JAX's collectives and lax.ppermute only.
A program may use at most 64 MiB of HBM per device.

```python
import math
import jax
import jax.numpy as jnp
from jax import lax

NS = 768
NF = 128
NT = 512
NFOC = 128
ITERS = 1
SRC_BLOCK = 96


def with_ends(values, own_key, low, high):
    index_at = [jax.random.randint(jax.random.fold_in(own_key, axis), (), 0, length) for axis, length in enumerate(values.shape)]
    main_axis = values.shape.index(max(values.shape))
    beside = index_at[:main_axis] + [(index_at[main_axis] + 1) % values.shape[main_axis]] + index_at[main_axis + 1:]
    return values.at[tuple(index_at)].set(low).at[tuple(beside)].set(high)


def shard_levels(rng, dims, split, least, largest):
    level = 1.0
    for dim, shards_of in split:
        draws = jax.random.uniform(jax.random.fold_in(jax.random.fold_in(rng, 6), dim), (shards_of,), jnp.float32, least / len(split), largest / len(split))
        level = level * jnp.repeat(jnp.exp(draws), dims[dim] // shards_of).reshape((-1,) + (1,) * (len(dims) - 1 - dim))
    return level


def bell_draw(stream_key, dims, spread, reach, split=(), held_as=jnp.bfloat16):
    entries = spread * jax.random.normal(stream_key, dims, jnp.float32)
    if split:
        entries = entries * shard_levels(stream_key, dims, split, -0.22, 0.18)
    return jnp.clip(entries, -reach, reach).astype(held_as)


def setup_inputs(seed: int = 0) -> dict:
    seeds = jax.random.split(jax.random.key(seed), 4)
    return {
        "reflection": bell_draw(seeds[0], (2, NF, NS, NS), NS ** -0.5, 0.21875, ((1, 32), (2, 8))),
        "direct": bell_draw(seeds[1], (NS, NFOC, NT), 1.0, 6.0, ((0, 256),)),
        "onset": with_ends(jax.random.randint(seeds[2], (NS, NFOC), NT // 4, 3 * NT // 4), jax.random.fold_in(seeds[2], 1), NT // 4, (3 * NT // 4) - 1).astype(jnp.int32),
    }


def lookup_tables():
    sample = jnp.arange(NT, dtype=jnp.int32)
    spectral_bin_index = jnp.arange(NF, dtype=jnp.int32)
    phase_index = sample[:, None] * spectral_bin_index[None, :] % NT
    angles = 2.0 * math.pi / NT * phase_index.astype(jnp.float32)
    cosine = jnp.cos(angles)
    sine = jnp.sin(angles)
    forward = (jnp.stack([cosine, -sine], axis=1) / math.sqrt(NT)).astype(jnp.bfloat16)
    inverse = (jnp.stack([cosine.T, -sine.T], axis=0) * (2.0 / math.sqrt(NT))).astype(jnp.bfloat16)
    return (forward, inverse)

def fourier_spectrum(field, forward):
    result = jnp.einsum('sqt,tcf->scfq', field.astype(jnp.float32), forward.astype(jnp.float32))
    return result.astype(jnp.bfloat16)

def apply_reflection(spectra, reflection, conj_sign):
    block_count = NS // SRC_BLOCK
    refl_blocks = reflection.reshape(2, NF, block_count, SRC_BLOCK, NS).transpose(2, 0, 1, 3, 4)
    spec_blocks = spectra.reshape(block_count, SRC_BLOCK, 2, NF, NFOC)

    def accumulate(summed, blocks):
        refl_block, spec_block = blocks
        refl_real = refl_block[0].astype(jnp.float32)
        refl_imag = refl_block[1].astype(jnp.float32)
        spectrum_real_rows = spec_block[:, 0].astype(jnp.float32)
        spec_imag = spec_block[:, 1].astype(jnp.float32)

        def product(left_operand, right_operand):
            return jnp.einsum('key,ekn->ykn', left_operand, right_operand)
        real_part = product(refl_real, spectrum_real_rows) - conj_sign * product(refl_imag, spec_imag)
        imag_part = product(refl_real, spec_imag) + conj_sign * product(refl_imag, spectrum_real_rows)
        rounded = jnp.stack([real_part, imag_part], axis=1).astype(jnp.bfloat16)
        rounded = lax.optimization_barrier(rounded)
        return (summed + rounded.astype(jnp.float32), None)
    start = jnp.zeros((NS, 2, NF, NFOC), jnp.float32)
    summed, _ = lax.scan(accumulate, start, (refl_blocks, spec_blocks))
    return summed

def inverse_window(summed, onset, inverse):
    traces = jnp.einsum('scfq,cft->sqt', summed.astype(jnp.float32), inverse.astype(jnp.float32))
    sample = jnp.arange(NT, dtype=jnp.int32)
    window = (sample[None, None, :] < onset[:, :, None]).astype(jnp.float32)
    return traces * window

def reference(reflection, direct, onset):
    forward, inverse = lookup_tables()
    focus_plus = direct
    focus_minus = direct
    minus_spectrum = fourier_spectrum(direct, forward)
    for sweep in range(ITERS):
        plus_spectrum = fourier_spectrum(focus_plus, forward)
        summed = apply_reflection(plus_spectrum, reflection, 1.0).astype(jnp.bfloat16)
        focus_minus = inverse_window(summed, onset, inverse).astype(jnp.bfloat16)
        minus_spectrum = fourier_spectrum(focus_minus, forward)
        summed = apply_reflection(minus_spectrum, reflection, -1.0).astype(jnp.bfloat16)
        focus_plus = (direct.astype(jnp.float32) + inverse_window(summed, onset, inverse)).astype(jnp.bfloat16)
    plus_spectrum = fourier_spectrum(focus_plus, forward)
    green_field = (apply_reflection(plus_spectrum, reflection, 1.0) - minus_spectrum.astype(jnp.float32)).astype(jnp.bfloat16)
    green_real = green_field[:, 0].astype(jnp.float32)
    green_imag = green_field[:, 1].astype(jnp.float32)
    real_part = jnp.einsum('rfa,rfb->fab', green_real, green_real) + jnp.einsum('rfa,rfb->fab', green_imag, green_imag)
    imag_part = jnp.einsum('rfa,rfb->fab', green_real, green_imag) - jnp.einsum('rfa,rfb->fab', green_imag, green_real)
    correlation = jnp.stack([real_part, imag_part], axis=0) / NS
    return (focus_plus, focus_minus, correlation)
```

```python
import functools
import math

import jax
import jax.numpy as jnp
import ml_dtypes
import numpy as np
from jax import lax
from jax.experimental import pallas as pl
from jax.experimental.pallas import tpu as pltpu
from jax.sharding import Mesh
from jax.sharding import PartitionSpec as P

F32 = jnp.float32
BF16 = jnp.bfloat16
RCV = ("xh", "y")
OWNERS = ("xh", "y", "freq")
TRACES = ("y", "freq")


def fourier_table(samples, bins_of_owner):
    phase = (bins_of_owner[:, None] * np.arange(samples)[None, :]) % samples
    angle = 2.0 * math.pi / samples * phase
    rows = np.concatenate([np.cos(angle), -np.sin(angle)], axis=0) / math.sqrt(samples)
    return rows.astype(np.float32).astype(ml_dtypes.bfloat16)


def dot(a, b, da, db):
    return lax.dot_general(a, b, (((da,), (db,)), ((), ())), preferred_element_type=F32)


def run(kernel, out, scratch, *args):
    return pl.pallas_call(
        kernel,
        out_shape=out,
        in_specs=[pl.BlockSpec(memory_space=pltpu.VMEM)] * len(args),
        out_specs=jax.tree.map(lambda _: pl.BlockSpec(memory_space=pltpu.VMEM), out),
        scratch_shapes=scratch,
        compiler_params=pltpu.CompilerParams(vmem_limit_bytes=32 * 2**20),
    )(*args)


def put_spectrum(field, table, rows_ref, i, step, conj):
    n = table.shape[0] // 2
    v = dot(table, field, 1, 1)
    rows_ref[pl.ds(2 * i, n, stride=step), :] = v[:n]
    im = v[n:]
    rows_ref[pl.ds(2 * i + 1, n, stride=step), :] = -im if conj else im


def flush(rows_ref, send_ref):
    rows = rows_ref[...].astype(BF16)
    for h in range(send_ref.shape[0]):
        send_ref[h] = rows


def first_kernel(direct_ref, table_ref, send_ref, out_rows):
    n = direct_ref.shape[0]
    for i in range(n):
        put_spectrum(direct_ref[i], table_ref[...], out_rows, i, 2 * n, False)
    flush(out_rows, send_ref)


def trace_kernel(n, conj_in, conj_out, add, *refs):
    if add:
        got_ref, onset_ref, table_ref, direct_ref, field_ref, send_ref, in_rows, out_rows = refs
    else:
        got_ref, onset_ref, table_ref, field_ref, send_ref, in_rows, out_rows = refs
    table = table_ref[...]
    bins = table.shape[0] // 2
    step = 2 * n
    in_rows[...] = got_ref[...].astype(F32)
    for i in range(n):
        re = in_rows[pl.ds(2 * i, bins, stride=step), :]
        im = in_rows[pl.ds(2 * i + 1, bins, stride=step), :]
        both = jnp.concatenate([re, -im if conj_in else im], axis=0).astype(BF16)
        trace = dot(both, table, 0, 0) * 2.0
        sample = lax.broadcasted_iota(jnp.int32, trace.shape, 1)
        trace = jnp.where(sample < onset_ref[:, i : i + 1], trace, 0.0)
        if add:
            trace = direct_ref[i].astype(F32) + trace
        field = trace.astype(BF16)
        field_ref[i] = field
        put_spectrum(field, table, out_rows, i, step, conj_out)
    flush(out_rows, send_ref)


def weave_kernel(got_ref, w_ref, even_odd):
    peers, _, block, half = got_ref.shape
    lanes = even_odd.shape[1]
    for col in range(0, half, lanes):
        for out, parts in ((0, (0, 1)), (1, (1, 0))):
            for b in range(peers):
                first, second = (got_ref[b, c, :, col : col + lanes].astype(F32) for c in parts)
                start = 2 * b * block
                even_odd[pl.ds(start, block, stride=2), :] = first
                even_odd[pl.ds(start + 1, block, stride=2), :] = second if out else -second
            at = out * half + col
            w_ref[:, at : at + lanes] = even_odd[...].astype(BF16)


def product(v_ref, w_ref):
    return dot(v_ref[...], w_ref[...], 0, 0).T


def apply_kernel(v_ref, w_ref, send_ref, rows):
    p = product(v_ref, w_ref)
    half = p.shape[0] // 2
    rows[pl.ds(0, half, stride=2), :] = p[:half]
    rows[pl.ds(1, half, stride=2), :] = p[half:]
    send_ref[...] = rows[...].astype(BF16)


def green_kernel(scale, v_ref, w_ref, minus_ref, corr_ref, rows):
    rows[...] = minus_ref[...].astype(F32)
    p = product(v_ref, w_ref)
    half = p.shape[0] // 2
    re = (p[:half] - rows[pl.ds(0, half, stride=2), :]).astype(BF16)
    im = (p[half:] + rows[pl.ds(1, half, stride=2), :]).astype(BF16)
    cross = dot(re, im, 0, 0)
    corr_ref[0] = ((dot(re, re, 0, 0) + dot(im, im, 0, 0)) * scale).astype(BF16)
    corr_ref[1] = ((cross - cross.T) * scale).astype(BF16)


def exchange(value, axes):
    return lax.all_to_all(value, axes, split_axis=0, concat_axis=0, tiled=True)


def on_device(reflection, direct, onset):
    n, focal, samples = direct.shape
    per_group = reflection.shape[1]
    block, receivers = reflection.shape[2:]
    halves, ys = lax.axis_size("xh"), lax.axis_size("y")
    groups = lax.axis_size("freq")
    bins = per_group * groups
    half = receivers // halves
    shape = jax.ShapeDtypeStruct

    order = (np.arange(groups)[None, :] * per_group + np.arange(ys)[:, None]).reshape(-1)
    table = jnp.asarray(fourier_table(samples, order))
    onset_cols = onset.T

    packed = reflection.reshape(2, per_group, block, halves, half).transpose(3, 1, 0, 2, 4)
    got = exchange(packed.reshape(halves * ys, 2, block, half), RCV)
    w = run(
        weave_kernel,
        shape((2 * receivers, 2 * half), BF16),
        [pltpu.VMEM((2 * receivers, focal), F32)],
        got,
    )

    rows_out = 2 * n * bins
    send_shape = shape((halves, rows_out, focal), BF16)
    field_shape = shape(direct.shape, BF16)
    rows = pltpu.VMEM((rows_out, focal), F32)

    def to_owners(send):
        parts = send.reshape(halves * bins, n, 2, focal)
        return exchange(parts, OWNERS).reshape(2 * receivers, focal)

    def to_traces(send):
        return exchange(send.reshape(bins, n, 2, focal), TRACES).reshape(rows_out, focal)

    def apply(v):
        return run(apply_kernel, shape((2 * half, focal), BF16), [pltpu.VMEM((2 * half, focal), F32)], v, w)

    plus = to_owners(run(first_kernel, send_shape, [rows], direct, table))
    summed = to_traces(apply(plus))
    focus_minus, send = run(
        functools.partial(trace_kernel, n, False, True, False),
        (field_shape, send_shape),
        [rows, rows],
        summed,
        onset_cols,
        table,
    )
    minus = to_owners(send)
    summed = to_traces(apply(minus))
    focus_plus, send = run(
        functools.partial(trace_kernel, n, True, False, True),
        (field_shape, send_shape),
        [rows, rows],
        summed,
        onset_cols,
        table,
        direct,
    )
    plus = to_owners(send)
    mine = lax.dynamic_index_in_dim(
        minus.reshape(halves, 2 * half, focal), lax.axis_index("xh"), 0, keepdims=False
    )
    partial = run(
        functools.partial(green_kernel, 1.0 / receivers),
        shape((2, focal, focal), BF16),
        [pltpu.VMEM((2 * half, focal), F32)],
        plus,
        w,
        mine,
    )
    rows_each = focal // (halves * ys)
    parts = partial.reshape(2, halves * ys, rows_each, focal).transpose(1, 0, 2, 3)
    arrived = exchange(parts, RCV).astype(F32)
    summed = arrived.reshape(halves, ys, 2, rows_each, focal).sum(axis=0)
    return focus_plus, focus_minus, summed.transpose(1, 0, 2, 3)


def solution(mesh):
    groups, rcv = mesh.shape["freq"], mesh.shape["rcv"]
    fine = Mesh(mesh.devices.reshape(groups, 2, rcv // 2), ("freq", "xh", "y"))
    traces = ("xh", "y", "freq")
    return jax.shard_map(
        on_device,
        mesh=fine,
        in_specs=(P(None, "freq", RCV, None), P(traces, None, None), P(traces, None)),
        out_specs=(P(traces, None, None), P(traces, None, None), P(None, "freq", RCV, None)),
        check_vma=False,
    )
```

```python
import functools
import math

import jax
import jax.numpy as jnp
import ml_dtypes
import numpy as np
from jax import lax
from jax.experimental import pallas as pl
from jax.experimental.pallas import tpu as pltpu
from jax.sharding import Mesh
from jax.sharding import PartitionSpec as P

F32 = jnp.float32
BF16 = jnp.bfloat16
RCV = ("xh", "y")
OWNERS = ("xh", "y", "freq")
TRACES = ("y", "freq")


def fourier_table(samples, bins_of_owner):
    phase = (bins_of_owner[:, None] * np.arange(samples)[None, :]) % samples
    angle = 2.0 * math.pi / samples * phase
    rows = np.concatenate([np.cos(angle), -np.sin(angle)], axis=0) / math.sqrt(samples)
    return rows.astype(np.float32).astype(ml_dtypes.bfloat16)


def dot(a, b, da, db):
    return lax.dot_general(a, b, (((da,), (db,)), ((), ())), preferred_element_type=F32)


def run(kernel, out, scratch, *args):
    return pl.pallas_call(
        kernel,
        out_shape=out,
        in_specs=[pl.BlockSpec(memory_space=pltpu.VMEM)] * len(args),
        out_specs=jax.tree.map(lambda _: pl.BlockSpec(memory_space=pltpu.VMEM), out),
        scratch_shapes=scratch,
        compiler_params=pltpu.CompilerParams(vmem_limit_bytes=32 * 2**20),
    )(*args)


def put_spectrum(field, table, rows_ref, i, step, conj):
    n = table.shape[0] // 2
    v = dot(table, field, 1, 1)
    rows_ref[pl.ds(2 * i, n, stride=step), :] = v[:n]
    im = v[n:]
    rows_ref[pl.ds(2 * i + 1, n, stride=step), :] = -im if conj else im


def flush(rows_ref, send_ref):
    rows = rows_ref[...].astype(BF16)
    for h in range(send_ref.shape[0]):
        send_ref[h] = rows


def first_kernel(direct_ref, table_ref, send_ref, out_rows):
    n = direct_ref.shape[0]
    for i in range(n):
        put_spectrum(direct_ref[i], table_ref[...], out_rows, i, 2 * n, False)
    flush(out_rows, send_ref)


def trace_kernel(n, conj_in, conj_out, add, *refs):
    if add:
        got_ref, onset_ref, table_ref, direct_ref, field_ref, send_ref, in_rows, out_rows = refs
    else:
        got_ref, onset_ref, table_ref, field_ref, send_ref, in_rows, out_rows = refs
    table = table_ref[...]
    bins = table.shape[0] // 2
    step = 2 * n
    in_rows[...] = got_ref[...].astype(F32)
    for i in range(n):
        re = in_rows[pl.ds(2 * i, bins, stride=step), :]
        im = in_rows[pl.ds(2 * i + 1, bins, stride=step), :]
        both = jnp.concatenate([re, -im if conj_in else im], axis=0).astype(BF16)
        trace = dot(both, table, 0, 0) * 2.0
        sample = lax.broadcasted_iota(jnp.int32, trace.shape, 1)
        square = (trace.shape[0], trace.shape[0])
        onset = jnp.broadcast_to(onset_ref[i : i + 1, :].astype(F32), square).T
        onset = jnp.concatenate([onset] * (trace.shape[1] // square[1]), axis=1)
        trace = jnp.where(sample.astype(F32) < onset, trace, 0.0)
        if add:
            trace = direct_ref[i].astype(F32) + trace
        field = trace.astype(BF16)
        field_ref[i] = field
        put_spectrum(field, table, out_rows, i, step, conj_out)
    flush(out_rows, send_ref)


def my_place():
    ys = lax.axis_size("y")
    return lax.axis_index("xh"), lax.axis_index("y"), ys


def pack_kernel(reflection_ref, *block_refs):
    half = block_refs[0].shape[2]
    xh, y, ys = my_place()
    for d, ref in enumerate(block_refs):
        start = pl.multiple_of(jnp.bitwise_xor(xh, d // ys) * half, half)
        ref[...] = reflection_ref[:, jnp.bitwise_xor(y, d % ys), :, pl.ds(start, half)]


def weave_kernel(*refs):
    *got_refs, w_ref, even_odd = refs
    _, block, half = got_refs[0].shape
    lanes = even_odd.shape[1]
    xh, y, ys = my_place()
    me = xh * ys + y
    for col in range(0, half, lanes):
        for out, parts in ((0, (0, 1)), (1, (1, 0))):
            for d, got_ref in enumerate(got_refs):
                first, second = (got_ref[c, :, col : col + lanes].astype(F32) for c in parts)
                start = 2 * block * jnp.bitwise_xor(me, d)
                even_odd[pl.ds(start, block, stride=2), :] = first
                even_odd[pl.ds(start + 1, block, stride=2), :] = second if out else -second
            at = out * half + col
            w_ref[:, at : at + lanes] = even_odd[...].astype(BF16)


def product(v_ref, w_ref):
    return dot(v_ref[...], w_ref[...], 0, 0).T


def apply_kernel(v_ref, w_ref, send_ref, rows):
    p = product(v_ref, w_ref)
    half = p.shape[0] // 2
    rows[pl.ds(0, half, stride=2), :] = p[:half]
    rows[pl.ds(1, half, stride=2), :] = p[half:]
    send_ref[...] = rows[...].astype(BF16)


def green_kernel(scale, v_ref, w_ref, minus_ref, corr_ref, rows):
    rows[...] = minus_ref[lax.axis_index("xh")].astype(F32)
    p = product(v_ref, w_ref)
    half = p.shape[0] // 2
    re = (p[:half] - rows[pl.ds(0, half, stride=2), :]).astype(BF16)
    im = (p[half:] + rows[pl.ds(1, half, stride=2), :]).astype(BF16)
    cross = dot(re, im, 0, 0)
    parts = (dot(re, re, 0, 0) + dot(im, im, 0, 0), cross - cross.T)
    peers, _, each, _ = corr_ref.shape
    for c, part in enumerate(parts):
        scaled = (part * scale).astype(BF16)
        for peer in range(peers):
            corr_ref[peer, c] = scaled[peer * each : (peer + 1) * each]


def total_kernel(got_ref, out_ref):
    bins = out_ref.shape[1]
    for c in range(out_ref.shape[0]):
        for k in range(bins):
            parts = [got_ref[at, c].astype(F32) for at in range(k, got_ref.shape[0], bins)]
            out_ref[c, k] = sum(parts[1:], parts[0])


def exchange(value, axes):
    return lax.all_to_all(value, axes, split_axis=0, concat_axis=0, tiled=True)


def on_device(reflection, direct, onset):
    n, focal, samples = direct.shape
    per_group = reflection.shape[1]
    block, receivers = reflection.shape[2:]
    halves, ys = lax.axis_size("xh"), lax.axis_size("y")
    groups = lax.axis_size("freq")
    bins = per_group * groups
    half = receivers // halves
    shape = jax.ShapeDtypeStruct

    order = (np.arange(groups)[None, :] * per_group + np.arange(ys)[:, None]).reshape(-1)
    table = jnp.asarray(fourier_table(samples, order))

    places = halves * ys
    piece = shape((2, block, half), BF16)
    mine, *others = run(pack_kernel, [piece] * places, [], reflection)
    got = [mine]
    for d, other in enumerate(others, 1):
        got.append(lax.ppermute(other, RCV, [(j, j ^ d) for j in range(places)]))
    w = run(
        weave_kernel,
        shape((2 * receivers, 2 * half), BF16),
        [pltpu.VMEM((2 * receivers, focal), F32)],
        *got,
    )

    rows_out = 2 * n * bins
    send_shape = shape((halves, rows_out, focal), BF16)
    field_shape = shape(direct.shape, BF16)
    rows = pltpu.VMEM((rows_out, focal), F32)

    def to_owners(send):
        parts = send.reshape(halves * bins, n, 2, focal)
        return exchange(parts, OWNERS).reshape(2 * receivers, focal)

    def to_traces(send):
        return exchange(send.reshape(bins, n, 2, focal), TRACES).reshape(rows_out, focal)

    def apply(v):
        return run(apply_kernel, shape((2 * half, focal), BF16), [pltpu.VMEM((2 * half, focal), F32)], v, w)

    plus = to_owners(run(first_kernel, send_shape, [rows], direct, table))
    summed = to_traces(apply(plus))
    focus_minus, send = run(
        functools.partial(trace_kernel, n, False, True, False),
        (field_shape, send_shape),
        [rows, rows],
        summed,
        onset,
        table,
    )
    minus = to_owners(send)
    summed = to_traces(apply(minus))
    focus_plus, send = run(
        functools.partial(trace_kernel, n, True, False, True),
        (field_shape, send_shape),
        [rows, rows],
        summed,
        onset,
        table,
        direct,
    )
    plus = to_owners(send)
    each = focal // places
    parts = run(
        functools.partial(green_kernel, 1.0 / receivers),
        shape((places, 2, each, focal), BF16),
        [pltpu.VMEM((2 * half, focal), F32)],
        plus,
        w,
        minus.reshape(halves, 2 * half, focal),
    )
    correlation = run(
        total_kernel, shape((2, per_group, each, focal), F32), [], exchange(parts, RCV)
    )
    return focus_plus, focus_minus, correlation


def solution(mesh):
    groups, rcv = mesh.shape["freq"], mesh.shape["rcv"]
    fine = Mesh(mesh.devices.reshape(groups, 2, rcv // 2), ("freq", "xh", "y"))
    traces = ("xh", "y", "freq")
    return jax.shard_map(
        on_device,
        mesh=fine,
        in_specs=(P(None, "freq", RCV, None), P(traces, None, None), P(traces, None)),
        out_specs=(P(traces, None, None), P(traces, None, None), P(None, "freq", RCV, None)),
        check_vma=False,
    )
```

```python
import functools
import math

import jax
import jax.numpy as jnp
import ml_dtypes
import numpy as np
from jax import lax
from jax.experimental import pallas as pl
from jax.experimental.pallas import tpu as pltpu
from jax.sharding import Mesh
from jax.sharding import PartitionSpec as P

F32 = jnp.float32
BF16 = jnp.bfloat16
RCV = ("xh", "y")
OWNERS = ("xh", "y", "freq")
TRACES = ("y", "freq")


def fourier_table(samples, bins_of_owner):
    phase = (bins_of_owner[:, None] * np.arange(samples)[None, :]) % samples
    angle = 2.0 * math.pi / samples * phase
    rows = np.concatenate([np.cos(angle), -np.sin(angle)], axis=0) / math.sqrt(samples)
    return rows.astype(np.float32).astype(ml_dtypes.bfloat16)


def dot(a, b, da, db):
    return lax.dot_general(a, b, (((da,), (db,)), ((), ())), preferred_element_type=F32)


def run(kernel, out, scratch, *args, space=pltpu.VMEM, out_spaces=None):
    if out_spaces is None:
        out_spaces = jax.tree.map(lambda _: pltpu.VMEM, out)
    return pl.pallas_call(
        kernel,
        out_shape=out,
        in_specs=[pl.BlockSpec(memory_space=space)] * len(args),
        out_specs=jax.tree.map(lambda at: pl.BlockSpec(memory_space=at), out_spaces),
        scratch_shapes=scratch,
        compiler_params=pltpu.CompilerParams(
            vmem_limit_bytes=(63 if space == pltpu.HBM else 12) * 2**20
        ),
    )(*args)


def put_spectrum(field, table, rows_ref, i, step, conj):
    n = table.shape[0] // 2
    v = dot(table, field, 1, 1)
    rows_ref[pl.ds(2 * i, n, stride=step), :] = v[:n]
    im = v[n:]
    rows_ref[pl.ds(2 * i + 1, n, stride=step), :] = -im if conj else im


def flush(rows_ref, send_ref):
    rows = rows_ref[...].astype(BF16)
    for h in range(send_ref.shape[0]):
        send_ref[h] = rows


def open_kernel(reflection_hbm, direct_hbm, table_hbm, *refs):
    *block_hbms, send_ref, blocks_ref, direct_ref, table_ref, out_rows, in_sems, out_sems = refs
    n = direct_hbm.shape[0]
    y = lax.axis_index("y")
    whole = pltpu.make_async_copy(table_hbm, table_ref, in_sems.at[0])
    parts = [
        pltpu.make_async_copy(direct_hbm.at[i], direct_ref.at[i], in_sems.at[1 + i])
        for i in range(n)
    ]
    takes, puts = [], []
    for d, block_hbm in enumerate(block_hbms):
        at = jnp.bitwise_xor(y, d)
        sem = in_sems.at[1 + n + d]
        takes.append(pltpu.make_async_copy(reflection_hbm.at[:, at], blocks_ref.at[d], sem))
        puts.append(pltpu.make_async_copy(blocks_ref.at[d], block_hbm, out_sems.at[d]))
    for copy in (whole, *parts, *takes):
        copy.start()
    whole.wait()
    for i in range(n):
        parts[i].wait()
        put_spectrum(direct_ref[i], table_ref[...], out_rows, i, 2 * n, False)
        if i == 0:
            for take, put in zip(takes, puts):
                take.wait()
                put.start()
    flush(out_rows, send_ref)
    for put in puts:
        put.wait()


def trace_kernel(n, conj_in, conj_out, add, *refs):
    if add:
        got_ref, onset_ref, table_ref, direct_ref, field_ref, send_ref, in_rows, out_rows = refs
    else:
        got_ref, onset_ref, table_ref, field_ref, send_ref, in_rows, out_rows = refs
    table = table_ref[...]
    bins = table.shape[0] // 2
    step = 2 * n
    in_rows[...] = sum(got_ref[h].astype(F32) for h in range(1, got_ref.shape[0])) + got_ref[0].astype(F32)
    for i in range(n):
        re = in_rows[pl.ds(2 * i, bins, stride=step), :]
        im = in_rows[pl.ds(2 * i + 1, bins, stride=step), :]
        both = jnp.concatenate([re, -im if conj_in else im], axis=0).astype(BF16)
        trace = dot(both, table, 0, 0) * 2.0
        sample = lax.broadcasted_iota(jnp.int32, trace.shape, 1)
        square = (trace.shape[0], trace.shape[0])
        onset = jnp.broadcast_to(onset_ref[i : i + 1, :].astype(F32), square).T
        onset = jnp.concatenate([onset] * (trace.shape[1] // square[1]), axis=1)
        trace = jnp.where(sample.astype(F32) < onset, trace, 0.0)
        if add:
            trace = direct_ref[i].astype(F32) + trace
        field = trace.astype(BF16)
        field_ref[i] = field
        put_spectrum(field, table, out_rows, i, step, conj_out)
    flush(out_rows, send_ref)


def weave(even_odd, pieces, negate):
    for start, even, odd in pieces:
        block = even.shape[0]
        even_odd[pl.ds(start, block, stride=2), :] = even.astype(F32)
        odd = odd.astype(F32)
        even_odd[pl.ds(start + 1, block, stride=2), :] = -odd if negate else odd
    return even_odd[...].astype(BF16)


def weave_sources_kernel(*refs):
    *got_refs, w_ref, cut_ref, even_odd = refs
    _, block, receivers = got_refs[0].shape
    lanes = even_odd.shape[1]
    half = cut_ref.shape[3]
    other = pl.multiple_of((1 - lax.axis_index("xh")) * half, half)
    for d, ref in enumerate(got_refs):
        cut_ref[d] = ref[:, :, pl.ds(other, half)]
    y = lax.axis_index("y")
    starts = [2 * block * jnp.bitwise_xor(y, d) for d in range(len(got_refs))]
    for out in (0, 1):
        for col in range(0, receivers, lanes):
            pieces = [
                (start, ref[out, :, col : col + lanes], ref[1 - out, :, col : col + lanes])
                for start, ref in zip(starts, got_refs)
            ]
            at = out * receivers + col
            w_ref[:, at : at + lanes] = weave(even_odd, pieces, not out)


def weave_far_kernel(cut_ref, w_ref, even_odd):
    places, _, block, half = cut_ref.shape
    lanes = even_odd.shape[1]
    y = lax.axis_index("y")
    starts = [2 * block * jnp.bitwise_xor(y, d) for d in range(places)]
    for out in (0, 1):
        for col in range(0, half, lanes):
            cols = slice(col, col + lanes)
            pieces = [
                (start, cut_ref[d, out, :, cols], cut_ref[d, 1 - out, :, cols])
                for d, start in enumerate(starts)
            ]
            at = out * half + col
            w_ref[:, at : at + lanes] = weave(even_odd, pieces, not out)


def product(v_ref, w_ref):
    return dot(v_ref[...], w_ref[...], 0, 0).T


def apply_kernel(v_ref, w_ref, send_ref, rows):
    p = product(v_ref, w_ref)
    half = p.shape[0] // 2
    rows[pl.ds(0, half, stride=2), :] = p[:half]
    rows[pl.ds(1, half, stride=2), :] = p[half:]
    send_ref[...] = rows[...].astype(BF16)


def green_kernel(scale, v_ref, w_ref, far_ref, minus_ref, corr_ref, rows):
    rows[...] = minus_ref[...].astype(F32)
    half = far_ref.shape[1] // 2
    receivers = w_ref.shape[1] // 2
    xh = lax.axis_index("xh")
    own, far = v_ref[xh], v_ref[1 - xh]

    def part(c):
        cols = pl.ds(pl.multiple_of(c * receivers + xh * half, half), half)
        near = dot(own, w_ref[:, cols], 0, 0)
        return (near + dot(far, far_ref[:, c * half : (c + 1) * half], 0, 0)).T

    re = (part(0) - rows[pl.ds(0, half, stride=2), :]).astype(BF16)
    im = (part(1) + rows[pl.ds(1, half, stride=2), :]).astype(BF16)
    cross = dot(re, im, 0, 0)
    parts = (dot(re, re, 0, 0) + dot(im, im, 0, 0), cross - cross.T)
    peers, _, each, _ = corr_ref.shape
    for c, part in enumerate(parts):
        scaled = (part * scale).astype(BF16)
        for peer in range(peers):
            corr_ref[peer, c] = scaled[peer * each : (peer + 1) * each]


def total_kernel(got_ref, out_ref):
    bins = out_ref.shape[1]
    for c in range(out_ref.shape[0]):
        for k in range(bins):
            parts = [got_ref[at, c].astype(F32) for at in range(k, got_ref.shape[0], bins)]
            out_ref[c, k] = sum(parts[1:], parts[0])


def exchange(value, axes):
    return lax.all_to_all(value, axes, split_axis=0, concat_axis=0, tiled=True)


def on_device(reflection, direct, onset):
    n, focal, samples = direct.shape
    per_group = reflection.shape[1]
    block, receivers = reflection.shape[2:]
    halves, ys = lax.axis_size("xh"), lax.axis_size("y")
    groups = lax.axis_size("freq")
    bins = per_group * groups
    half = receivers // halves
    shape = jax.ShapeDtypeStruct

    order = (np.arange(groups)[None, :] * per_group + np.arange(ys)[:, None]).reshape(-1)
    table = jnp.asarray(fourier_table(samples, order))

    places = halves * ys
    rows_out = 2 * n * bins
    field_shape = shape(direct.shape, BF16)
    rows = pltpu.VMEM((rows_out, focal), F32)

    def send_shape(copies):
        return shape((copies, rows_out, focal), BF16)

    def swap(value, axes):
        parts = value.reshape(-1, n, 2, focal)
        return exchange(parts, axes).reshape(-1, rows_out, focal)

    piece = shape((2, block, receivers), BF16)
    *got, send = run(
        open_kernel,
        [piece] * ys + [send_shape(1)],
        [
            pltpu.VMEM((ys, *piece.shape), BF16),
            pltpu.VMEM(direct.shape, BF16),
            pltpu.VMEM(table.shape, BF16),
            rows,
            pltpu.SemaphoreType.DMA((1 + n + ys,)),
            pltpu.SemaphoreType.DMA((ys,)),
        ],
        reflection,
        direct,
        table,
        space=pltpu.HBM,
        out_spaces=[pltpu.HBM] * ys + [pltpu.VMEM],
    )
    for d in range(1, ys):
        got[d] = lax.ppermute(got[d], "y", [(j, j ^ d) for j in range(ys)])
    plus = swap(send, TRACES)
    w, cut = run(
        weave_sources_kernel,
        (shape((2 * half, 2 * receivers), BF16), shape((ys, 2, block, half), BF16)),
        [pltpu.VMEM((2 * half, focal), F32)],
        *got,
    )
    far = lax.ppermute(cut, "xh", [(j, j ^ 1) for j in range(halves)])
    w_far = run(
        weave_far_kernel,
        shape((2 * half, 2 * half), BF16),
        [pltpu.VMEM((2 * half, focal), F32)],
        far,
    )

    def apply(v):
        out = run(
            apply_kernel,
            shape((2 * receivers, focal), BF16),
            [pltpu.VMEM((2 * receivers, focal), F32)],
            v.reshape(2 * half, focal),
            w,
        )
        return swap(out, OWNERS)

    summed = apply(plus)
    focus_minus, send = run(
        functools.partial(trace_kernel, n, False, True, False),
        (field_shape, send_shape(1)),
        [rows, rows],
        summed,
        onset,
        table,
    )
    minus = swap(send, TRACES)
    summed = apply(minus)
    focus_plus, send = run(
        functools.partial(trace_kernel, n, True, False, True),
        (field_shape, send_shape(halves)),
        [rows, rows],
        summed,
        onset,
        table,
        direct,
    )
    plus = swap(send, OWNERS)
    each = focal // places
    parts = run(
        functools.partial(green_kernel, 1.0 / receivers),
        shape((places, 2, each, focal), BF16),
        [pltpu.VMEM((2 * half, focal), F32)],
        plus,
        w,
        w_far,
        minus.reshape(2 * half, focal),
    )
    correlation = run(
        total_kernel, shape((2, per_group, each, focal), F32), [], exchange(parts, RCV)
    )
    return focus_plus, focus_minus, correlation


def solution(mesh):
    groups, rcv = mesh.shape["freq"], mesh.shape["rcv"]
    fine = Mesh(mesh.devices.reshape(groups, 2, rcv // 2), ("freq", "xh", "y"))
    traces = ("xh", "y", "freq")
    return jax.shard_map(
        on_device,
        mesh=fine,
        in_specs=(P(None, "freq", RCV, None), P(traces, None, None), P(traces, None)),
        out_specs=(P(traces, None, None), P(traces, None, None), P(None, "freq", RCV, None)),
        check_vma=False,
    )
```

```python
import functools
import math

import jax
import jax.numpy as jnp
import ml_dtypes
import numpy as np
from jax import lax
from jax.experimental import pallas as pl
from jax.experimental.pallas import tpu as pltpu
from jax.sharding import Mesh
from jax.sharding import PartitionSpec as P

F32 = jnp.float32
BF16 = jnp.bfloat16
RCV = ("xh", "y")
OWNERS = ("xh", "y", "freq")
TRACES = ("y", "freq")


def fourier_table(samples, bins_of_owner):
    phase = (bins_of_owner[:, None] * np.arange(samples)[None, :]) % samples
    angle = 2.0 * math.pi / samples * phase
    rows = np.concatenate([np.cos(angle), -np.sin(angle)], axis=0) / math.sqrt(samples)
    return rows.astype(np.float32).astype(ml_dtypes.bfloat16)


def dot(a, b, da, db):
    return lax.dot_general(a, b, (((da,), (db,)), ((), ())), preferred_element_type=F32)


def run(kernel, out, scratch, *args, space=pltpu.VMEM, out_spaces=None):
    if out_spaces is None:
        out_spaces = jax.tree.map(lambda _: pltpu.VMEM, out)
    return pl.pallas_call(
        kernel,
        out_shape=out,
        in_specs=[pl.BlockSpec(memory_space=space)] * len(args),
        out_specs=jax.tree.map(lambda at: pl.BlockSpec(memory_space=at), out_spaces),
        scratch_shapes=scratch,
        compiler_params=pltpu.CompilerParams(
            vmem_limit_bytes=(63 if space == pltpu.HBM else 12) * 2**20
        ),
    )(*args)


def put_spectrum(field, table, rows_ref, i, step, conj):
    n = table.shape[0] // 2
    v = dot(table, field, 1, 1)
    rows_ref[pl.ds(2 * i, n, stride=step), :] = v[:n]
    im = v[n:]
    rows_ref[pl.ds(2 * i + 1, n, stride=step), :] = -im if conj else im


def flush(rows_ref, send_ref):
    rows = rows_ref[...].astype(BF16)
    for h in range(send_ref.shape[0]):
        send_ref[h] = rows


def open_kernel(reflection_hbm, direct_hbm, table_hbm, *refs):
    *block_hbms, send_ref, blocks_ref, direct_ref, table_ref, out_rows, in_sems, out_sems = refs
    n = direct_hbm.shape[0]
    y = lax.axis_index("y")
    whole = pltpu.make_async_copy(table_hbm, table_ref, in_sems.at[0])
    parts = [
        pltpu.make_async_copy(direct_hbm.at[i], direct_ref.at[i], in_sems.at[1 + i])
        for i in range(n)
    ]
    takes, puts = [], []
    for d, block_hbm in enumerate(block_hbms):
        at = jnp.bitwise_xor(y, d)
        sem = in_sems.at[1 + n + d]
        takes.append(pltpu.make_async_copy(reflection_hbm.at[:, at], blocks_ref.at[d], sem))
        puts.append(pltpu.make_async_copy(blocks_ref.at[d], block_hbm, out_sems.at[d]))
    for copy in (whole, *parts, *takes):
        copy.start()
    whole.wait()
    for i in range(n):
        parts[i].wait()
        put_spectrum(direct_ref[i], table_ref[...], out_rows, i, 2 * n, False)
        if i == 0:
            for take, put in zip(takes, puts):
                take.wait()
                put.start()
    flush(out_rows, send_ref)
    for put in puts:
        put.wait()


def trace_kernel(n, conj_in, conj_out, add, *refs):
    got_ref, onset_ref, table_ref, *refs = refs
    direct_ref = refs.pop(0) if add else None
    field_hbm, send_ref, field_ref, in_rows, out_rows, sems = refs
    table = table_ref[...]
    bins = table.shape[0] // 2
    step = 2 * n
    summed = got_ref[0].astype(F32)
    for h in range(1, got_ref.shape[0]):
        summed += got_ref[h].astype(F32)
    in_rows[...] = summed
    for i in range(n):
        re = in_rows[pl.ds(2 * i, bins, stride=step), :]
        im = in_rows[pl.ds(2 * i + 1, bins, stride=step), :]
        both = jnp.concatenate([re, -im if conj_in else im], axis=0).astype(BF16)
        trace = dot(both, table, 0, 0) * 2.0
        sample = lax.broadcasted_iota(jnp.int32, trace.shape, 1)
        square = (trace.shape[0], trace.shape[0])
        onset = jnp.broadcast_to(onset_ref[i : i + 1, :].astype(F32), square).T
        onset = jnp.concatenate([onset] * (trace.shape[1] // square[1]), axis=1)
        trace = jnp.where(sample.astype(F32) < onset, trace, 0.0)
        if add:
            trace = direct_ref[i].astype(F32) + trace
        field_ref[i] = trace.astype(BF16)
    put_spectrum(field_ref[0], table, out_rows, 0, step, conj_out)
    copies = [pltpu.make_async_copy(field_ref.at[i], field_hbm.at[i], sems.at[i]) for i in range(n)]
    for copy in copies:
        copy.start()
    for i in range(1, n):
        put_spectrum(field_ref[i], table, out_rows, i, step, conj_out)
    flush(out_rows, send_ref)
    for copy in copies:
        copy.wait()


def weave(even_odd, pieces, negate):
    for start, even, odd in pieces:
        block = even.shape[0]
        even_odd[pl.ds(start, block, stride=2), :] = even.astype(F32)
        odd = odd.astype(F32)
        even_odd[pl.ds(start + 1, block, stride=2), :] = -odd if negate else odd
    return even_odd[...].astype(BF16)


def weave_sources_kernel(*refs):
    *got_refs, w_ref, cut_ref, even_odd = refs
    _, block, receivers = got_refs[0].shape
    lanes = even_odd.shape[1]
    half = cut_ref.shape[3]
    other = pl.multiple_of((1 - lax.axis_index("xh")) * half, half)
    for d, ref in enumerate(got_refs):
        cut_ref[d] = ref[:, :, pl.ds(other, half)]
    y = lax.axis_index("y")
    starts = [2 * block * jnp.bitwise_xor(y, d) for d in range(len(got_refs))]
    for out in (0, 1):
        for col in range(0, receivers, lanes):
            pieces = [
                (start, ref[out, :, col : col + lanes], ref[1 - out, :, col : col + lanes])
                for start, ref in zip(starts, got_refs)
            ]
            at = out * receivers + col
            w_ref[:, at : at + lanes] = weave(even_odd, pieces, not out)


def weave_far_kernel(cut_ref, w_ref, even_odd):
    places, _, block, half = cut_ref.shape
    lanes = even_odd.shape[1]
    y = lax.axis_index("y")
    starts = [2 * block * jnp.bitwise_xor(y, d) for d in range(places)]
    for out in (0, 1):
        for col in range(0, half, lanes):
            cols = slice(col, col + lanes)
            pieces = [
                (start, cut_ref[d, out, :, cols], cut_ref[d, 1 - out, :, cols])
                for d, start in enumerate(starts)
            ]
            at = out * half + col
            w_ref[:, at : at + lanes] = weave(even_odd, pieces, not out)


def product(v_ref, w_ref):
    return dot(v_ref[...], w_ref[...], 0, 0).T


def apply_kernel(v_ref, w_ref, send_ref, rows):
    p = product(v_ref, w_ref)
    half = p.shape[0] // 2
    rows[pl.ds(0, half, stride=2), :] = p[:half]
    rows[pl.ds(1, half, stride=2), :] = p[half:]
    send_ref[...] = rows[...].astype(BF16)


def green_kernel(scale, v_ref, w_ref, far_ref, minus_ref, corr_ref, rows):
    rows[...] = minus_ref[...].astype(F32)
    half = far_ref.shape[1] // 2
    receivers = w_ref.shape[1] // 2
    xh = lax.axis_index("xh")
    own, far = v_ref[xh], v_ref[1 - xh]

    def part(c):
        cols = pl.ds(pl.multiple_of(c * receivers + xh * half, half), half)
        near = dot(own, w_ref[:, cols], 0, 0)
        return (near + dot(far, far_ref[:, c * half : (c + 1) * half], 0, 0)).T

    re = (part(0) - rows[pl.ds(0, half, stride=2), :]).astype(BF16)
    im = (part(1) + rows[pl.ds(1, half, stride=2), :]).astype(BF16)
    cross = dot(re, im, 0, 0)
    parts = (dot(re, re, 0, 0) + dot(im, im, 0, 0), cross - cross.T)
    peers, _, each, _ = corr_ref.shape
    for c, part in enumerate(parts):
        scaled = (part * scale).astype(BF16)
        for peer in range(peers):
            corr_ref[peer, c] = scaled[peer * each : (peer + 1) * each]


def total_kernel(got_ref, out_ref):
    bins = out_ref.shape[1]
    for c in range(out_ref.shape[0]):
        for k in range(bins):
            parts = [got_ref[at, c].astype(F32) for at in range(k, got_ref.shape[0], bins)]
            out_ref[c, k] = sum(parts[1:], parts[0])


def exchange(value, axes):
    return lax.all_to_all(value, axes, split_axis=0, concat_axis=0, tiled=True)


def on_device(reflection, direct, onset):
    n, focal, samples = direct.shape
    per_group = reflection.shape[1]
    block, receivers = reflection.shape[2:]
    halves, ys = lax.axis_size("xh"), lax.axis_size("y")
    groups = lax.axis_size("freq")
    bins = per_group * groups
    half = receivers // halves
    shape = jax.ShapeDtypeStruct

    order = (np.arange(groups)[None, :] * per_group + np.arange(ys)[:, None]).reshape(-1)
    table = jnp.asarray(fourier_table(samples, order))

    places = halves * ys
    rows_out = 2 * n * bins
    field_shape = shape(direct.shape, BF16)
    rows = pltpu.VMEM((rows_out, focal), F32)

    def send_shape(copies):
        return shape((copies, rows_out, focal), BF16)

    def swap(value, axes):
        parts = value.reshape(-1, n, 2, focal)
        return exchange(parts, axes).reshape(-1, rows_out, focal)

    piece = shape((2, block, receivers), BF16)
    *got, send = run(
        open_kernel,
        [piece] * ys + [send_shape(1)],
        [
            pltpu.VMEM((ys, *piece.shape), BF16),
            pltpu.VMEM(direct.shape, BF16),
            pltpu.VMEM(table.shape, BF16),
            rows,
            pltpu.SemaphoreType.DMA((1 + n + ys,)),
            pltpu.SemaphoreType.DMA((ys,)),
        ],
        reflection,
        direct,
        table,
        space=pltpu.HBM,
        out_spaces=[pltpu.HBM] * ys + [pltpu.VMEM],
    )
    for d in range(1, ys):
        got[d] = lax.ppermute(got[d], "y", [(j, j ^ d) for j in range(ys)])
    plus = swap(send, TRACES)
    w, cut = run(
        weave_sources_kernel,
        (shape((2 * half, 2 * receivers), BF16), shape((ys, 2, block, half), BF16)),
        [pltpu.VMEM((2 * half, focal), F32)],
        *got,
    )
    far = lax.ppermute(cut, "xh", [(j, j ^ 1) for j in range(halves)])

    def apply(v):
        out = run(
            apply_kernel,
            shape((2 * receivers, focal), BF16),
            [pltpu.VMEM((2 * receivers, focal), F32)],
            v.reshape(2 * half, focal),
            w,
        )
        return swap(out, OWNERS)

    def to_field(summed, conj, copies, *extra):
        return run(
            functools.partial(trace_kernel, n, not conj, conj, bool(extra)),
            (field_shape, send_shape(copies)),
            [pltpu.VMEM(direct.shape, BF16), rows, rows, pltpu.SemaphoreType.DMA((n,))],
            summed,
            onset,
            table,
            *extra,
            out_spaces=(pltpu.HBM, pltpu.VMEM),
        )

    summed = apply(plus)
    focus_minus, send = to_field(summed, True, 1)
    send, far = lax.optimization_barrier((send, far))
    w_far = run(
        weave_far_kernel,
        shape((2 * half, 2 * half), BF16),
        [pltpu.VMEM((2 * half, focal), F32)],
        far,
    )
    send, w_far = lax.optimization_barrier((send, w_far))
    minus = swap(send, TRACES)
    summed = apply(minus)
    focus_plus, send = to_field(summed, False, halves, direct)
    plus = swap(send, OWNERS)
    each = focal // places
    parts = run(
        functools.partial(green_kernel, 1.0 / receivers),
        shape((places, 2, each, focal), BF16),
        [pltpu.VMEM((2 * half, focal), F32)],
        plus,
        w,
        w_far,
        minus.reshape(2 * half, focal),
    )
    correlation = run(
        total_kernel, shape((2, per_group, each, focal), F32), [], exchange(parts, RCV)
    )
    return focus_plus, focus_minus, correlation


def solution(mesh):
    groups, rcv = mesh.shape["freq"], mesh.shape["rcv"]
    fine = Mesh(mesh.devices.reshape(groups, 2, rcv // 2), ("freq", "xh", "y"))
    traces = ("xh", "y", "freq")
    return jax.shard_map(
        on_device,
        mesh=fine,
        in_specs=(P(None, "freq", RCV, None), P(traces, None, None), P(traces, None)),
        out_specs=(P(traces, None, None), P(traces, None, None), P(None, "freq", RCV, None)),
        check_vma=False,
    )
```

```python
import functools
import math

import jax
import jax.numpy as jnp
import ml_dtypes
import numpy as np
from jax import lax
from jax.experimental import pallas as pl
from jax.experimental.pallas import tpu as pltpu
from jax.sharding import Mesh
from jax.sharding import PartitionSpec as P

F32 = jnp.float32
BF16 = jnp.bfloat16
RCV = ("xh", "y")
OWNERS = ("xh", "y", "freq")
TRACES = ("y", "freq")


def fourier_table(samples, bins_of_owner):
    phase = (bins_of_owner[:, None] * np.arange(samples)[None, :]) % samples
    angle = 2.0 * math.pi / samples * phase
    rows = np.concatenate([np.cos(angle), -np.sin(angle)], axis=0) / math.sqrt(samples)
    return rows.astype(np.float32).astype(ml_dtypes.bfloat16)


def dot(a, b, da, db):
    return lax.dot_general(a, b, (((da,), (db,)), ((), ())), preferred_element_type=F32)


def run(kernel, out, scratch, *args, space=pltpu.VMEM, out_spaces=None):
    if out_spaces is None:
        out_spaces = jax.tree.map(lambda _: pltpu.VMEM, out)
    return pl.pallas_call(
        kernel,
        out_shape=out,
        in_specs=[pl.BlockSpec(memory_space=space)] * len(args),
        out_specs=jax.tree.map(lambda at: pl.BlockSpec(memory_space=at), out_spaces),
        scratch_shapes=scratch,
        compiler_params=pltpu.CompilerParams(
            vmem_limit_bytes=(63 if space == pltpu.HBM else 12) * 2**20
        ),
    )(*args)


def put_spectrum(field, table, rows_ref, i, step, conj):
    n = table.shape[0] // 2
    v = dot(table, field, 1, 1)
    rows_ref[pl.ds(2 * i, n, stride=step), :] = v[:n]
    im = v[n:]
    rows_ref[pl.ds(2 * i + 1, n, stride=step), :] = -im if conj else im


def flush(rows_ref, send_ref):
    rows = rows_ref[...].astype(BF16)
    for h in range(send_ref.shape[0]):
        send_ref[h] = rows


def open_kernel(reflection_hbm, direct_hbm, table_hbm, *refs):
    *block_hbms, send_ref, blocks_ref, direct_ref, table_ref, out_rows, in_sems, out_sems = refs
    n = direct_hbm.shape[0]
    y = lax.axis_index("y")
    whole = pltpu.make_async_copy(table_hbm, table_ref, in_sems.at[0])
    parts = [
        pltpu.make_async_copy(direct_hbm.at[i], direct_ref.at[i], in_sems.at[1 + i])
        for i in range(n)
    ]
    takes, puts = [], []
    for d, block_hbm in enumerate(block_hbms):
        at = jnp.bitwise_xor(y, d)
        sem = in_sems.at[1 + n + d]
        takes.append(pltpu.make_async_copy(reflection_hbm.at[:, at], blocks_ref.at[d], sem))
        puts.append(pltpu.make_async_copy(blocks_ref.at[d], block_hbm, out_sems.at[d]))
    for copy in (whole, *parts, *takes):
        copy.start()
    whole.wait()
    for i in range(n):
        parts[i].wait()
        put_spectrum(direct_ref[i], table_ref[...], out_rows, i, 2 * n, False)
        if i == 0:
            for take, put in zip(takes, puts):
                take.wait()
                put.start()
    flush(out_rows, send_ref)
    for put in puts:
        put.wait()


def trace_kernel(n, conj_in, conj_out, add, *refs):
    got_ref, onset_ref, table_ref, *refs = refs
    direct_ref = refs.pop(0) if add else None
    field_ref, send_ref, in_rows, out_rows = refs
    table = table_ref[...]
    bins = table.shape[0] // 2
    step = 2 * n
    summed = got_ref[0].astype(F32)
    for h in range(1, got_ref.shape[0]):
        summed += got_ref[h].astype(F32)
    in_rows[...] = summed
    for i in range(n):
        re = in_rows[pl.ds(2 * i, bins, stride=step), :]
        im = in_rows[pl.ds(2 * i + 1, bins, stride=step), :]
        both = jnp.concatenate([re, -im if conj_in else im], axis=0).astype(BF16)
        trace = dot(both, table, 0, 0) * 2.0
        sample = lax.broadcasted_iota(jnp.int32, trace.shape, 1)
        square = (trace.shape[0], trace.shape[0])
        onset = jnp.broadcast_to(onset_ref[i : i + 1, :].astype(F32), square).T
        onset = jnp.concatenate([onset] * (trace.shape[1] // square[1]), axis=1)
        trace = jnp.where(sample.astype(F32) < onset, trace, 0.0)
        if add:
            trace = direct_ref[i].astype(F32) + trace
        field_ref[i] = trace.astype(BF16)
        put_spectrum(field_ref[i], table, out_rows, i, step, conj_out)
    flush(out_rows, send_ref)


def weave(even_odd, pieces, negate):
    for start, even, odd in pieces:
        block = even.shape[0]
        even_odd[pl.ds(start, block, stride=2), :] = even.astype(F32)
        odd = odd.astype(F32)
        even_odd[pl.ds(start + 1, block, stride=2), :] = -odd if negate else odd
    return even_odd[...].astype(BF16)


def weave_sources_kernel(*refs):
    *got_refs, w_ref, cut_ref, even_odd = refs
    _, block, receivers = got_refs[0].shape
    lanes = even_odd.shape[1]
    half = cut_ref.shape[3]
    other = pl.multiple_of((1 - lax.axis_index("xh")) * half, half)
    for d, ref in enumerate(got_refs):
        cut_ref[d] = ref[:, :, pl.ds(other, half)]
    y = lax.axis_index("y")
    starts = [2 * block * jnp.bitwise_xor(y, d) for d in range(len(got_refs))]
    for out in (0, 1):
        for col in range(0, receivers, lanes):
            pieces = [
                (start, ref[out, :, col : col + lanes], ref[1 - out, :, col : col + lanes])
                for start, ref in zip(starts, got_refs)
            ]
            at = out * receivers + col
            w_ref[:, at : at + lanes] = weave(even_odd, pieces, not out)


def weave_far_kernel(cut_ref, w_ref, even_odd):
    places, _, block, half = cut_ref.shape
    lanes = even_odd.shape[1]
    y = lax.axis_index("y")
    starts = [2 * block * jnp.bitwise_xor(y, d) for d in range(places)]
    for out in (0, 1):
        for col in range(0, half, lanes):
            cols = slice(col, col + lanes)
            pieces = [
                (start, cut_ref[d, out, :, cols], cut_ref[d, 1 - out, :, cols])
                for d, start in enumerate(starts)
            ]
            at = out * half + col
            w_ref[:, at : at + lanes] = weave(even_odd, pieces, not out)


def product(v_ref, w_ref):
    return dot(v_ref[...], w_ref[...], 0, 0).T


def apply_kernel(v_ref, w_ref, send_ref, rows):
    p = product(v_ref, w_ref)
    half = p.shape[0] // 2
    rows[pl.ds(0, half, stride=2), :] = p[:half]
    rows[pl.ds(1, half, stride=2), :] = p[half:]
    send_ref[...] = rows[...].astype(BF16)


def green_kernel(scale, *refs):
    v_ref, w_ref, far_ref, minus_ref, *fields, corr_ref, plus_hbm, minus_hbm, rows, sems = refs
    copies = [
        pltpu.make_async_copy(field, hbm, sems.at[i])
        for i, (field, hbm) in enumerate(zip(fields, (plus_hbm, minus_hbm)))
    ]
    for copy in copies:
        copy.start()
    rows[...] = minus_ref[...].astype(F32)
    half = far_ref.shape[1] // 2
    receivers = w_ref.shape[1] // 2
    xh = lax.axis_index("xh")
    own, far = v_ref[xh], v_ref[1 - xh]

    def part(c):
        cols = pl.ds(pl.multiple_of(c * receivers + xh * half, half), half)
        near = dot(own, w_ref[:, cols], 0, 0)
        return (near + dot(far, far_ref[:, c * half : (c + 1) * half], 0, 0)).T

    re = (part(0) - rows[pl.ds(0, half, stride=2), :]).astype(BF16)
    im = (part(1) + rows[pl.ds(1, half, stride=2), :]).astype(BF16)
    cross = dot(re, im, 0, 0)
    parts = (dot(re, re, 0, 0) + dot(im, im, 0, 0), cross - cross.T)
    peers, _, each, _ = corr_ref.shape
    for c, part in enumerate(parts):
        scaled = (part * scale).astype(BF16)
        for peer in range(peers):
            corr_ref[peer, c] = scaled[peer * each : (peer + 1) * each]
    for copy in copies:
        copy.wait()


def total_kernel(got_ref, out_ref):
    bins = out_ref.shape[1]
    for c in range(out_ref.shape[0]):
        for k in range(bins):
            parts = [got_ref[at, c].astype(F32) for at in range(k, got_ref.shape[0], bins)]
            out_ref[c, k] = sum(parts[1:], parts[0])


def exchange(value, axes):
    return lax.all_to_all(value, axes, split_axis=0, concat_axis=0, tiled=True)


def on_device(reflection, direct, onset):
    n, focal, samples = direct.shape
    per_group = reflection.shape[1]
    block, receivers = reflection.shape[2:]
    halves, ys = lax.axis_size("xh"), lax.axis_size("y")
    groups = lax.axis_size("freq")
    bins = per_group * groups
    half = receivers // halves
    shape = jax.ShapeDtypeStruct

    order = (np.arange(groups)[None, :] * per_group + np.arange(ys)[:, None]).reshape(-1)
    table = jnp.asarray(fourier_table(samples, order))

    places = halves * ys
    rows_out = 2 * n * bins
    field_shape = shape(direct.shape, BF16)
    rows = pltpu.VMEM((rows_out, focal), F32)

    def send_shape(copies):
        return shape((copies, rows_out, focal), BF16)

    def swap(value, axes):
        parts = value.reshape(-1, n, 2, focal)
        return exchange(parts, axes).reshape(-1, rows_out, focal)

    piece = shape((2, block, receivers), BF16)
    *got, send = run(
        open_kernel,
        [piece] * ys + [send_shape(1)],
        [
            pltpu.VMEM((ys, *piece.shape), BF16),
            pltpu.VMEM(direct.shape, BF16),
            pltpu.VMEM(table.shape, BF16),
            rows,
            pltpu.SemaphoreType.DMA((1 + n + ys,)),
            pltpu.SemaphoreType.DMA((ys,)),
        ],
        reflection,
        direct,
        table,
        space=pltpu.HBM,
        out_spaces=[pltpu.HBM] * ys + [pltpu.VMEM],
    )
    for d in range(1, ys):
        got[d] = lax.ppermute(got[d], "y", [(j, j ^ d) for j in range(ys)])
    plus = swap(send, TRACES)
    w, cut = run(
        weave_sources_kernel,
        (shape((2 * half, 2 * receivers), BF16), shape((ys, 2, block, half), BF16)),
        [pltpu.VMEM((2 * half, focal), F32)],
        *got,
    )
    far = lax.ppermute(cut, "xh", [(j, j ^ 1) for j in range(halves)])

    def apply(v):
        out = run(
            apply_kernel,
            shape((2 * receivers, focal), BF16),
            [pltpu.VMEM((2 * receivers, focal), F32)],
            v.reshape(2 * half, focal),
            w,
        )
        return swap(out, OWNERS)

    def to_field(summed, conj, copies, *extra):
        return run(
            functools.partial(trace_kernel, n, not conj, conj, bool(extra)),
            (field_shape, send_shape(copies)),
            [rows, rows],
            summed,
            onset,
            table,
            *extra,
        )

    summed = apply(plus)
    focus_minus, send = to_field(summed, True, 1)
    send, far = lax.optimization_barrier((send, far))
    w_far = run(
        weave_far_kernel,
        shape((2 * half, 2 * half), BF16),
        [pltpu.VMEM((2 * half, focal), F32)],
        far,
    )
    send, w_far = lax.optimization_barrier((send, w_far))
    minus = swap(send, TRACES)
    summed = apply(minus)
    focus_plus, send = to_field(summed, False, halves, direct)
    plus = swap(send, OWNERS)
    each = focal // places
    parts, focus_plus, focus_minus = run(
        functools.partial(green_kernel, 1.0 / receivers),
        (shape((places, 2, each, focal), BF16), field_shape, field_shape),
        [pltpu.VMEM((2 * half, focal), F32), pltpu.SemaphoreType.DMA((2,))],
        plus,
        w,
        w_far,
        minus.reshape(2 * half, focal),
        focus_plus,
        focus_minus,
        out_spaces=(pltpu.VMEM, pltpu.HBM, pltpu.HBM),
    )
    correlation = run(
        total_kernel, shape((2, per_group, each, focal), F32), [], exchange(parts, RCV)
    )
    return focus_plus, focus_minus, correlation


def solution(mesh):
    groups, rcv = mesh.shape["freq"], mesh.shape["rcv"]
    fine = Mesh(mesh.devices.reshape(groups, 2, rcv // 2), ("freq", "xh", "y"))
    traces = ("xh", "y", "freq")
    return jax.shard_map(
        on_device,
        mesh=fine,
        in_specs=(P(None, "freq", RCV, None), P(traces, None, None), P(traces, None)),
        out_specs=(P(traces, None, None), P(traces, None, None), P(None, "freq", RCV, None)),
        check_vma=False,
    )
```

```python
import functools
import math

import jax
import jax.numpy as jnp
import ml_dtypes
import numpy as np
from jax import lax
from jax.experimental import pallas as pl
from jax.experimental.pallas import tpu as pltpu
from jax.sharding import Mesh
from jax.sharding import PartitionSpec as P

F32 = jnp.float32
BF16 = jnp.bfloat16
RCV = ("xh", "y")
OWNERS = ("xh", "y", "freq")
TRACES = ("y", "freq")


def fourier_table(samples, bins_of_owner):
    phase = (bins_of_owner[:, None] * np.arange(samples)[None, :]) % samples
    angle = 2.0 * math.pi / samples * phase
    rows = np.concatenate([np.cos(angle), -np.sin(angle)], axis=0) / math.sqrt(samples)
    return rows.astype(np.float32).astype(ml_dtypes.bfloat16)


def dot(a, b, da, db):
    return lax.dot_general(a, b, (((da,), (db,)), ((), ())), preferred_element_type=F32)


def run(kernel, out, scratch, *args, space=pltpu.VMEM, out_spaces=None):
    if out_spaces is None:
        out_spaces = jax.tree.map(lambda _: pltpu.VMEM, out)
    return pl.pallas_call(
        kernel,
        out_shape=out,
        in_specs=[pl.BlockSpec(memory_space=space)] * len(args),
        out_specs=jax.tree.map(lambda at: pl.BlockSpec(memory_space=at), out_spaces),
        scratch_shapes=scratch,
        compiler_params=pltpu.CompilerParams(
            vmem_limit_bytes=(63 if space == pltpu.HBM else 12) * 2**20
        ),
    )(*args)


def put_spectrum(field, table, rows_ref, i, step, conj):
    n = table.shape[0] // 2
    v = dot(table, field, 1, 1)
    rows_ref[pl.ds(2 * i, n, stride=step), :] = v[:n]
    im = v[n:]
    rows_ref[pl.ds(2 * i + 1, n, stride=step), :] = -im if conj else im


def flush(rows_ref, send_ref):
    rows = rows_ref[...].astype(BF16)
    for h in range(send_ref.shape[0]):
        send_ref[h] = rows


def open_kernel(reflection_hbm, direct_hbm, table_hbm, *refs):
    *block_hbms, send_ref, blocks_ref, direct_ref, table_ref, out_rows, in_sems, out_sems = refs
    n = direct_hbm.shape[0]
    y = lax.axis_index("y")
    whole = pltpu.make_async_copy(table_hbm, table_ref, in_sems.at[0])
    parts = [
        pltpu.make_async_copy(direct_hbm.at[i], direct_ref.at[i], in_sems.at[1 + i])
        for i in range(n)
    ]
    takes, puts = [], []
    for d, block_hbm in enumerate(block_hbms):
        at = jnp.bitwise_xor(y, d + 1)
        sem = in_sems.at[1 + n + d]
        takes.append(pltpu.make_async_copy(reflection_hbm.at[:, at], blocks_ref.at[d], sem))
        puts.append(pltpu.make_async_copy(blocks_ref.at[d], block_hbm, out_sems.at[d]))
    for copy in (*takes, whole, *parts):
        copy.start()
    for take, put in zip(takes, puts):
        take.wait()
        put.start()
    whole.wait()
    for i in range(n):
        parts[i].wait()
        put_spectrum(direct_ref[i], table_ref[...], out_rows, i, 2 * n, False)
    flush(out_rows, send_ref)
    for put in puts:
        put.wait()


def trace_kernel(n, conj_in, conj_out, add, *refs):
    got_ref, onset_ref, table_ref, *refs = refs
    direct_ref = refs.pop(0) if add else None
    field_ref, send_ref, in_rows, out_rows = refs
    table = table_ref[...]
    bins = table.shape[0] // 2
    step = 2 * n
    summed = got_ref[0].astype(F32)
    for h in range(1, got_ref.shape[0]):
        summed += got_ref[h].astype(F32)
    in_rows[...] = summed
    for i in range(n):
        re = in_rows[pl.ds(2 * i, bins, stride=step), :]
        im = in_rows[pl.ds(2 * i + 1, bins, stride=step), :]
        both = jnp.concatenate([re, -im if conj_in else im], axis=0).astype(BF16)
        trace = dot(both, table, 0, 0) * 2.0
        sample = lax.broadcasted_iota(jnp.int32, trace.shape, 1)
        square = (trace.shape[0], trace.shape[0])
        onset = jnp.broadcast_to(onset_ref[i : i + 1, :].astype(F32), square).T
        onset = jnp.concatenate([onset] * (trace.shape[1] // square[1]), axis=1)
        trace = jnp.where(sample.astype(F32) < onset, trace, 0.0)
        if add:
            trace = direct_ref[i].astype(F32) + trace
        field_ref[i] = trace.astype(BF16)
        put_spectrum(field_ref[i], table, out_rows, i, step, conj_out)
    flush(out_rows, send_ref)


def weave(even_odd, pieces, negate):
    for start, even, odd in pieces:
        block = even.shape[0]
        even_odd[pl.ds(start, block, stride=2), :] = even.astype(F32)
        odd = odd.astype(F32)
        even_odd[pl.ds(start + 1, block, stride=2), :] = -odd if negate else odd
    return even_odd[...].astype(BF16)


def weave_sources_kernel(*refs):
    reflection_ref, *got_refs, w_ref, cut_ref, even_odd = refs
    _, block, receivers = got_refs[0].shape
    lanes = even_odd.shape[1]
    half = cut_ref.shape[3]
    other = pl.multiple_of((1 - lax.axis_index("xh")) * half, half)
    y = lax.axis_index("y")
    got_refs = [reflection_ref.at[:, y], *got_refs]
    for d, ref in enumerate(got_refs):
        cut_ref[d] = ref[:, :, pl.ds(other, half)]
    starts = [2 * block * jnp.bitwise_xor(y, d) for d in range(len(got_refs))]
    for out in (0, 1):
        for col in range(0, receivers, lanes):
            pieces = [
                (start, ref[out, :, col : col + lanes], ref[1 - out, :, col : col + lanes])
                for start, ref in zip(starts, got_refs)
            ]
            at = out * receivers + col
            w_ref[:, at : at + lanes] = weave(even_odd, pieces, not out)


def weave_far_kernel(cut_ref, w_ref, even_odd):
    places, _, block, half = cut_ref.shape
    lanes = even_odd.shape[1]
    y = lax.axis_index("y")
    starts = [2 * block * jnp.bitwise_xor(y, d) for d in range(places)]
    for out in (0, 1):
        for col in range(0, half, lanes):
            cols = slice(col, col + lanes)
            pieces = [
                (start, cut_ref[d, out, :, cols], cut_ref[d, 1 - out, :, cols])
                for d, start in enumerate(starts)
            ]
            at = out * half + col
            w_ref[:, at : at + lanes] = weave(even_odd, pieces, not out)


def product(v_ref, w_ref):
    return dot(v_ref[...], w_ref[...], 0, 0).T


def apply_kernel(v_ref, w_ref, send_ref, rows):
    p = product(v_ref, w_ref)
    half = p.shape[0] // 2
    rows[pl.ds(0, half, stride=2), :] = p[:half]
    rows[pl.ds(1, half, stride=2), :] = p[half:]
    send_ref[...] = rows[...].astype(BF16)


def green_kernel(scale, *refs):
    v_ref, w_ref, far_ref, minus_ref, *fields, corr_ref, plus_hbm, minus_hbm, rows, sems = refs
    copies = [
        pltpu.make_async_copy(field, hbm, sems.at[i])
        for i, (field, hbm) in enumerate(zip(fields, (plus_hbm, minus_hbm)))
    ]
    for copy in copies:
        copy.start()
    rows[...] = minus_ref[...].astype(F32)
    half = far_ref.shape[1] // 2
    receivers = w_ref.shape[1] // 2
    xh = lax.axis_index("xh")
    own, far = v_ref[xh], v_ref[1 - xh]

    def part(c):
        cols = pl.ds(pl.multiple_of(c * receivers + xh * half, half), half)
        near = dot(own, w_ref[:, cols], 0, 0)
        return near + dot(far, far_ref[:, c * half : (c + 1) * half], 0, 0)

    minus_re, minus_im = rows[pl.ds(0, half, stride=2), :].T, rows[pl.ds(1, half, stride=2), :].T
    re = (part(0) - minus_re).astype(BF16)
    im = (part(1) + minus_im).astype(BF16)
    cross = dot(re, im, 1, 1)
    parts = (dot(re, re, 1, 1) + dot(im, im, 1, 1), cross - cross.T)
    peers, _, each, _ = corr_ref.shape
    for c, part in enumerate(parts):
        scaled = (part * scale).astype(BF16)
        for peer in range(peers):
            corr_ref[peer, c] = scaled[peer * each : (peer + 1) * each]
    for copy in copies:
        copy.wait()


def total_kernel(got_ref, out_ref):
    bins = out_ref.shape[1]
    for c in range(out_ref.shape[0]):
        for k in range(bins):
            parts = [got_ref[at, c].astype(F32) for at in range(k, got_ref.shape[0], bins)]
            out_ref[c, k] = sum(parts[1:], parts[0])


def exchange(value, axes):
    return lax.all_to_all(value, axes, split_axis=0, concat_axis=0, tiled=True)


def on_device(reflection, direct, onset):
    n, focal, samples = direct.shape
    per_group = reflection.shape[1]
    block, receivers = reflection.shape[2:]
    halves, ys = lax.axis_size("xh"), lax.axis_size("y")
    groups = lax.axis_size("freq")
    bins = per_group * groups
    half = receivers // halves
    shape = jax.ShapeDtypeStruct

    order = (np.arange(groups)[None, :] * per_group + np.arange(ys)[:, None]).reshape(-1)
    table = jnp.asarray(fourier_table(samples, order))

    places = halves * ys
    rows_out = 2 * n * bins
    field_shape = shape(direct.shape, BF16)
    rows = pltpu.VMEM((rows_out, focal), F32)

    def send_shape(copies):
        return shape((copies, rows_out, focal), BF16)

    def swap(value, axes):
        parts = value.reshape(-1, n, 2, focal)
        return exchange(parts, axes).reshape(-1, rows_out, focal)

    piece = shape((2, block, receivers), BF16)
    *got, send = run(
        open_kernel,
        [piece] * (ys - 1) + [send_shape(1)],
        [
            pltpu.VMEM((ys - 1, *piece.shape), BF16),
            pltpu.VMEM(direct.shape, BF16),
            pltpu.VMEM(table.shape, BF16),
            rows,
            pltpu.SemaphoreType.DMA((n + ys,)),
            pltpu.SemaphoreType.DMA((ys - 1,)),
        ],
        reflection,
        direct,
        table,
        space=pltpu.HBM,
        out_spaces=[pltpu.HBM] * (ys - 1) + [pltpu.VMEM],
    )
    for d in range(1, ys):
        got[d - 1] = lax.ppermute(got[d - 1], "y", [(j, j ^ d) for j in range(ys)])
    plus = swap(send, TRACES)
    w, cut = run(
        weave_sources_kernel,
        (shape((2 * half, 2 * receivers), BF16), shape((ys, 2, block, half), BF16)),
        [pltpu.VMEM((2 * half, focal), F32)],
        reflection,
        *got,
    )
    far = lax.ppermute(cut, "xh", [(j, j ^ 1) for j in range(halves)])

    def apply(v):
        out = run(
            apply_kernel,
            shape((2 * receivers, focal), BF16),
            [pltpu.VMEM((2 * receivers, focal), F32)],
            v.reshape(2 * half, focal),
            w,
        )
        return swap(out, OWNERS)

    def to_field(summed, conj, copies, *extra):
        return run(
            functools.partial(trace_kernel, n, not conj, conj, bool(extra)),
            (field_shape, send_shape(copies)),
            [rows, rows],
            summed,
            onset,
            table,
            *extra,
        )

    summed = apply(plus)
    focus_minus, send = to_field(summed, True, 1)
    send, far = lax.optimization_barrier((send, far))
    w_far = run(
        weave_far_kernel,
        shape((2 * half, 2 * half), BF16),
        [pltpu.VMEM((2 * half, focal), F32)],
        far,
    )
    send, w_far = lax.optimization_barrier((send, w_far))
    minus = swap(send, TRACES)
    summed = apply(minus)
    focus_plus, send = to_field(summed, False, halves, direct)
    plus = swap(send, OWNERS)
    each = focal // places
    parts, focus_plus, focus_minus = run(
        functools.partial(green_kernel, 1.0 / receivers),
        (shape((places, 2, each, focal), BF16), field_shape, field_shape),
        [pltpu.VMEM((2 * half, focal), F32), pltpu.SemaphoreType.DMA((2,))],
        plus,
        w,
        w_far,
        minus.reshape(2 * half, focal),
        focus_plus,
        focus_minus,
        out_spaces=(pltpu.VMEM, pltpu.HBM, pltpu.HBM),
    )
    correlation = run(
        total_kernel, shape((2, per_group, each, focal), F32), [], exchange(parts, RCV)
    )
    return focus_plus, focus_minus, correlation


def solution(mesh):
    groups, rcv = mesh.shape["freq"], mesh.shape["rcv"]
    fine = Mesh(mesh.devices.reshape(groups, 2, rcv // 2), ("freq", "xh", "y"))
    traces = ("xh", "y", "freq")
    return jax.shard_map(
        on_device,
        mesh=fine,
        in_specs=(P(None, "freq", RCV, None), P(traces, None, None), P(traces, None)),
        out_specs=(P(traces, None, None), P(traces, None, None), P(None, "freq", RCV, None)),
        check_vma=False,
    )
```
